32 devices in a mesh: rows: 2 (over x), ci: 4 (over z), cj: 4 (over y, core).
Axes of the slice: x: 2, y: 2, z: 4, core: 2. Of those that a mesh axis runs over, the one named last changes fastest.
Arguments:
- matrix: float32 [512, 49152], P('rows', ('ci', 'cj')), may hold values from -585 to 585
- sample: int32 [4, 4, 512], P('ci', None, 'rows'), may hold values 0 or 1
Outputs:
- cosine: float32 [4, 12288, 4, 384], P('ci', 'rows', 'cj')
The draws below stay inside these ranges and needn't reach their ends.
All inputs are finite; a program needn't handle non-finite values. No bound on the sum of `sample` on one device may be relied on, other than what follows from the above.
Results may differ from the reference program's by a relative error of at most 0.000054.
Values sent between devices are 32-bit elements; how exact they have to be, the bound alone decides.
A program may use at most 128 MiB of HBM per device.

```python
import math
import jax
import jax.numpy as jnp
from jax import lax

COLUMNS = 49152
TOTAL_ROWS = 512
SLAB = 3072
BLOCK = 12288
QSLAB = 96
QGROUP = 384
N_CI = 4
N_CJ = 4


def draw_matrix(key, part):
    keys = jax.random.split(jax.random.fold_in(key, 17), 4)
    position = jnp.arange(TOTAL_ROWS, dtype=jnp.float32)
    rising = 1.0 + 2.0 * position / TOTAL_ROWS
    col_scale = jnp.exp(jax.random.uniform(keys[1], (COLUMNS,), jnp.float32, 0.0, math.log(10.0)))
    shared = jnp.clip(jax.random.normal(keys[2], (TOTAL_ROWS,), jnp.float32), -4.0, 4.0)
    loading = jax.random.uniform(keys[3], (COLUMNS,), jnp.float32, -1.2, 1.2)
    noise = jnp.clip(jax.random.normal(keys[0], (TOTAL_ROWS, COLUMNS), jnp.float32), -6.0, 6.0)
    return rising[:, None] * (noise + shared[:, None] * loading[None, :]) * col_scale[None, :]


def with_ends(values, own_key, smallest, high):
    longest = values.shape.index(max(values.shape))
    spots = []
    for shift in (0, 1):
        where = [jax.random.randint(jax.random.fold_in(own_key, axis), (), 0, length) for axis, length in enumerate(values.shape)]
        where[longest] = (where[longest] + shift) % values.shape[longest]
        spots.append(tuple(where))
    return values.at[spots[0]].set(smallest).at[spots[1]].set(high)


def setup_inputs(seed: int = 0) -> dict:
    seeds = jax.random.split(jax.random.key(seed), 3)
    return {
        "matrix": draw_matrix(jax.random.fold_in(seeds[2], 71), 0),
        "sample": with_ends((jax.random.randint(seeds[1], (N_CI, N_CJ, TOTAL_ROWS), 0, 2) < 1).astype(jnp.int32), jax.random.fold_in(seeds[1], 1), 0, 1),
    }


EPS = 1e-06
KEEP = 2.0

def reference(matrix, sample):
    inverse = 1.0 / jnp.sqrt(lax.optimization_barrier(jnp.sum(matrix * matrix, axis=0)) + EPS)
    unit = matrix * inverse[None, :]
    query = unit.reshape(TOTAL_ROWS, N_CI, N_CJ, SLAB)[:, :, :, :QSLAB]
    query = jnp.transpose(query, (0, 2, 1, 3)).reshape(TOTAL_ROWS, N_CJ, QGROUP) * KEEP
    blocks = unit.reshape(TOTAL_ROWS, N_CI, BLOCK)

    def one_block(index):
        columns = lax.dynamic_index_in_dim(blocks, index, 1, keepdims=False)
        picks = lax.dynamic_index_in_dim(sample, index, 0, keepdims=False).astype(jnp.float32)
        masked = query * jnp.transpose(picks)[:, :, None]
        product = jnp.dot(jnp.transpose(columns), masked.reshape(TOTAL_ROWS, N_CJ * QGROUP), precision=lax.Precision.HIGHEST, preferred_element_type=jnp.float32)
        return product.reshape(BLOCK, N_CJ, QGROUP)
    return lax.map(one_block, jnp.arange(N_CI, dtype=jnp.int32))
```

```python
import functools

import jax
import jax.numpy as jnp
from jax import lax
from jax.experimental import pallas as pl
from jax.experimental.pallas import tpu as pltpu
from jax.sharding import PartitionSpec as P

QUERY = 1536


EPS = 1e-06
KEEP = 2.0

WIDTH = 128
AHEAD = 4
MESH = pl.DeviceIdType.MESH


def shards(matrix, sample):
    local_squares = jnp.sum(matrix * matrix, axis=0)
    total_squares = lax.psum(local_squares, "rows")
    inverse = 1.0 / jnp.sqrt(total_squares + EPS)
    unit = matrix * inverse[None, :]
    count_ci = lax.axis_size("ci")
    count_cj = lax.axis_size("cj")
    count_rows = lax.axis_size("rows")
    row_count = matrix.shape[0]
    query_slab = QUERY // (count_ci * count_cj)
    queries = unit[:, :query_slab] * KEEP
    swapped = lax.all_to_all(unit, "cj", split_axis=0, concat_axis=1, tiled=True)
    ranged = lax.all_to_all(swapped, "rows", split_axis=1, concat_axis=0, tiled=True)
    columns = lax.all_gather(ranged, "cj", axis=0, tiled=True)
    picks = lax.dynamic_index_in_dim(sample[0], lax.axis_index("cj"), 0, keepdims=False).astype(
        jnp.float32
    )
    part_group = lax.all_gather(queries, "ci", axis=1, tiled=True) * picks[:, None]
    masked = lax.all_gather(part_group, "rows", axis=0, tiled=True)
    group_width = masked.shape[1]
    reordered = masked.reshape(count_rows, count_cj, row_count // count_cj, group_width)
    reordered = jnp.transpose(reordered, (1, 0, 2, 3)).reshape(count_rows * row_count, group_width)
    result = jnp.dot(
        jnp.transpose(columns),
        reordered,
        precision=lax.Precision.HIGHEST,
        preferred_element_type=jnp.float32,
    )
    return result[None, :, None, :]


def split(value):
    high = value.astype(jnp.bfloat16)
    low = (value - high.astype(jnp.float32)).astype(jnp.bfloat16)
    return high, low


def kernel(
    count_ci, chunks, query_slab,
    mat_ref, sample_ref, out_ref,
    buf, xb, pa, px, qa, qx, sx, qmat, stage,
    load_sem, y_send, y_recv, x_send, x_recv, a_send, a_recv, f_send, f_recv,
    q_load, qx_sems, sx_sems, qa_send, qa_recv, qz_send, qz_recv, out_sem,
):
    x, z, cj = lax.axis_index("rows"), lax.axis_index("ci"), lax.axis_index("cj")
    y, core = cj // 2, cj % 2
    off = (x + y) % 2
    rows = mat_ref.shape[0]
    slab = chunks * WIDTH
    group = out_ref.shape[1]
    x_peer = (1 - x, z, cj)
    y_peer = (x, z, (1 - y) * 2 + core)
    twin = (x, z, y * 2 + 1 - core)

    def z_peer(d):
        return (x, (z + d) % count_ci, cj)

    def remote(src, dst, send, recv, device):
        return pltpu.make_async_remote_copy(
            src_ref=src, dst_ref=dst, send_sem=send, recv_sem=recv,
            device_id=device, device_id_type=MESH,
        )

    def load(c):
        start = c * WIDTH
        if not isinstance(c, int):
            start = pl.multiple_of(start, WIDTH)
        return pltpu.make_async_copy(
            mat_ref.at[:, pl.ds(start, WIDTH)], buf.at[0, c], load_sem.at[c]
        )

    def y_copy(c):
        return remote(buf.at[0, c], buf.at[1, c], y_send.at[c], y_recv.at[c], y_peer)

    def x_copy(c):
        return remote(buf.at[1 - off, c], xb.at[c], x_send.at[c], x_recv.at[c], x_peer)

    def a_copy(c):
        return remote(buf.at[off, c], pa.at[c], a_send.at[c], a_recv.at[c], twin)

    def f_copy(c):
        return remote(xb.at[c], px.at[c], f_send.at[c], f_recv.at[c], twin)

    q_in = pltpu.make_async_copy(mat_ref.at[:, pl.ds(0, WIDTH)], qa.at[z], q_load)
    q_in.start()
    for c in range(chunks):
        load(c).start()

    barrier = pltpu.get_barrier_semaphore()
    peers = [x_peer, y_peer, twin] + [z_peer(d) for d in range(1, count_ci)]
    for peer in peers:
        pl.semaphore_signal(barrier, inc=1, device_id=peer, device_id_type=MESH)
    pl.semaphore_wait(barrier, len(peers))

    qx_copy = remote(qa.at[z], qx.at[z], qx_sems.at[0], qx_sems.at[1], x_peer)
    sx_copy = remote(sample_ref, sx, sx_sems.at[0], sx_sems.at[1], x_peer)

    def qa_copy(d, slot):
        return remote(qa.at[z], qa.at[slot], qa_send.at[d], qa_recv.at[d], z_peer(d))

    def qz_copy(d, slot):
        return remote(qx.at[z], qx.at[slot], qz_send.at[d], qz_recv.at[d], z_peer(d))

    def send_own(c):
        load(c).wait()
        y_copy(c).start()

        @pl.when(off == 1)
        def _():
            x_copy(c).start()

    q_in.wait()
    qx_copy.start()
    for c in range(AHEAD):
        send_own(c)
    sx_copy.start()
    for d in range(1, count_ci):
        qa_copy(d, z).start()
    qx_copy.wait_recv()
    for d in range(1, count_ci):
        qz_copy(d, z).start()

    def relay(c):
        y_copy(c).wait_recv()

        @pl.when(off == 0)
        def _():
            x_copy(c).start()

        a_copy(c).start()

        @pl.when(c + AHEAD < chunks)
        def _():
            send_own(c + AHEAD)

    def forward(c):
        x_copy(c).wait_recv()
        f_copy(c).start()

    def out_copy(k, part):
        home = core if part == 0 else 1 - core
        start = pl.multiple_of(home * slab + k * WIDTH, WIDTH)
        return pltpu.make_async_copy(
            stage.at[k, part], out_ref.at[pl.ds(start, WIDTH), :], out_sem.at[k, part]
        )

    def compute(k):
        a_copy(k).wait_recv()
        f_copy(k).wait_recv()
        own = jnp.concatenate([jnp.transpose(buf[off, k]), jnp.transpose(xb[k])], axis=1)
        other = jnp.concatenate([jnp.transpose(pa[k]), jnp.transpose(px[k])], axis=1)
        both = jnp.concatenate([own, other], axis=0)
        squares = jnp.sum(both * both, axis=1, keepdims=True)
        inverse = 1.0 / jnp.sqrt(squares + EPS)
        high, low = split(both)
        left = jnp.concatenate([high, low, high], axis=1)
        product = jnp.dot(left, qmat[...], preferred_element_type=jnp.float32) * inverse
        for part in range(2):
            stage[k, part] = product[part * WIDTH:(part + 1) * WIDTH]
            out_copy(k, part).start()

    def prepare():
        for d in range(1, count_ci):
            slot = (z + count_ci - d) % count_ci
            qa_copy(d, slot).wait_recv()
            qz_copy(d, slot).wait_recv()
        sx_copy.wait_recv()
        inverses = []
        for i in range(count_ci):
            first, second = qa[i], qx[i]
            squares = jnp.sum(first * first, axis=0, keepdims=True)
            squares += jnp.sum(second * second, axis=0, keepdims=True)
            inverses.append(1.0 / jnp.sqrt(squares + EPS))
        lane = lax.broadcasted_iota(jnp.int32, (rows, WIDTH), 1)
        for half, (pieces, picks) in enumerate(((qa, sample_ref), (qx, sx))):
            row = picks[pl.ds(cj, 1), :].astype(jnp.float32)
            mask = jnp.transpose(jnp.broadcast_to(row, (WIDTH, rows)))
            tiles = [jnp.zeros((rows, WIDTH), jnp.float32)] * (group // WIDTH)
            for i in range(count_ci):
                value = pieces[i] * inverses[i] * KEEP * mask
                first = i * query_slab
                if first % WIDTH:
                    value = pltpu.roll(value, first % WIDTH, 1)
                for t in range(first // WIDTH, (first + query_slab - 1) // WIDTH + 1):
                    low_lane, high_lane = first - t * WIDTH, first + query_slab - t * WIDTH
                    tiles[t] = jnp.where((lane >= low_lane) & (lane < high_lane), value, tiles[t])
            for t, tile in enumerate(tiles):
                high, low = split(tile)
                where = slice(t * WIDTH, (t + 1) * WIDTH)
                for third, piece in enumerate((high, high, low)):
                    base = third * 2 * rows + half * rows
                    qmat[base:base + rows, where] = piece

    lag = chunks * 5 // 12

    relay(0)

    @pl.loop(1, lag)
    def _(c):
        relay(c)
        forward(c - 1)

    prepare()

    @pl.loop(lag, 2 * lag - 2)
    def _(c):
        relay(c)
        forward(c - 1)

        @pl.loop(0, 2)
        def _(s):
            compute(2 * (c - lag) + s)

    @pl.loop(2 * lag - 2, chunks)
    def _(c):
        relay(c)
        forward(c - 1)
        compute(c - 2)

    forward(chunks - 1)

    @pl.loop(chunks - 2, chunks)
    def _(k):
        compute(k)

    @pl.loop(0, chunks)
    def _(c):
        y_copy(c).wait_send()
        x_copy(c).wait_send()
        a_copy(c).wait_send()
        f_copy(c).wait_send()
        out_copy(c, 0).wait()
        out_copy(c, 1).wait()

    qx_copy.wait_send()
    sx_copy.wait_send()
    for d in range(1, count_ci):
        qa_copy(d, z).wait_send()
        qz_copy(d, z).wait_send()


def fused(matrix, sample):
    count_ci, count_cj = lax.axis_size("ci"), lax.axis_size("cj")
    rows, slab = matrix.shape
    query_slab = QUERY // (count_ci * count_cj)
    group = query_slab * count_ci
    chunks = slab // WIDTH
    dma = pltpu.SemaphoreType.DMA
    blocks = pltpu.VMEM((chunks, rows, WIDTH), jnp.float32)
    pieces = pltpu.VMEM((count_ci, rows, WIDTH), jnp.float32)
    result = pl.pallas_call(
        functools.partial(kernel, count_ci, chunks, query_slab),
        out_shape=jax.ShapeDtypeStruct((2 * slab, group), jnp.float32),
        in_specs=[
            pl.BlockSpec(memory_space=pl.ANY),
            pl.BlockSpec(memory_space=pltpu.VMEM),
        ],
        out_specs=pl.BlockSpec(memory_space=pl.ANY),
        scratch_shapes=[
            pltpu.VMEM((2, chunks, rows, WIDTH), jnp.float32),
            blocks, blocks, blocks, pieces, pieces,
            pltpu.VMEM(sample.shape[1:], sample.dtype),
            pltpu.VMEM((6 * rows, group), jnp.bfloat16),
            pltpu.VMEM((chunks, 2, WIDTH, group), jnp.float32),
        ] + [dma((chunks,))] * 9 + [dma, dma((2,)), dma((2,))] + [dma((count_ci,))] * 4
        + [dma((chunks, 2))],
        compiler_params=pltpu.CompilerParams(
            collective_id=0, has_side_effects=True, vmem_limit_bytes=63 * 2**20
        ),
    )(matrix, sample[0])
    return result[None, :, None, :]


def solution(mesh):
    in_specs = (P("rows", ("ci", "cj")), P("ci", None, "rows"))
    out_specs = P("ci", "rows", "cj", None)
    body = fused if mesh.shape["rows"] == 2 and mesh.shape["cj"] == 4 else shards
    return jax.shard_map(body, mesh=mesh, in_specs=in_specs, out_specs=out_specs, check_vma=False)
```

```python
import functools

import jax
import jax.numpy as jnp
from jax import lax
from jax.experimental import pallas as pl
from jax.experimental.pallas import tpu as pltpu
from jax.sharding import PartitionSpec as P

QUERY = 1536


EPS = 1e-06
KEEP = 2.0

WIDTH = 128
AHEAD = 4
MESH = pl.DeviceIdType.MESH


def shards(matrix, sample):
    local_squares = jnp.sum(matrix * matrix, axis=0)
    total_squares = lax.psum(local_squares, "rows")
    inverse = 1.0 / jnp.sqrt(total_squares + EPS)
    unit = matrix * inverse[None, :]
    count_ci = lax.axis_size("ci")
    count_cj = lax.axis_size("cj")
    count_rows = lax.axis_size("rows")
    row_count = matrix.shape[0]
    query_slab = QUERY // (count_ci * count_cj)
    queries = unit[:, :query_slab] * KEEP
    swapped = lax.all_to_all(unit, "cj", split_axis=0, concat_axis=1, tiled=True)
    ranged = lax.all_to_all(swapped, "rows", split_axis=1, concat_axis=0, tiled=True)
    columns = lax.all_gather(ranged, "cj", axis=0, tiled=True)
    picks = lax.dynamic_index_in_dim(sample[0], lax.axis_index("cj"), 0, keepdims=False).astype(
        jnp.float32
    )
    part_group = lax.all_gather(queries, "ci", axis=1, tiled=True) * picks[:, None]
    masked = lax.all_gather(part_group, "rows", axis=0, tiled=True)
    group_width = masked.shape[1]
    reordered = masked.reshape(count_rows, count_cj, row_count // count_cj, group_width)
    reordered = jnp.transpose(reordered, (1, 0, 2, 3)).reshape(count_rows * row_count, group_width)
    result = jnp.dot(
        jnp.transpose(columns),
        reordered,
        precision=lax.Precision.HIGHEST,
        preferred_element_type=jnp.float32,
    )
    return result[None, :, None, :]


def split(value):
    high = value.astype(jnp.bfloat16)
    low = (value - high.astype(jnp.float32)).astype(jnp.bfloat16)
    return high, low


def kernel(
    count_ci, chunks, query_slab,
    mat_ref, sample_ref, out_ref,
    buf, xb, pa, px, qa, qx, sx, qmat,
    load_sem, y_send, y_recv, x_send, x_recv, a_send, a_recv, f_send, f_recv,
    q_load, qx_sems, sx_sems, qa_send, qa_recv, qz_send, qz_recv,
):
    x, z, cj = lax.axis_index("rows"), lax.axis_index("ci"), lax.axis_index("cj")
    y, core = cj // 2, cj % 2
    off = (x + y) % 2
    rows = mat_ref.shape[0]
    slab = chunks * WIDTH
    group = query_slab * count_ci
    part_rows = rows // 2
    x_peer = (1 - x, z, cj)
    y_peer = (x, z, (1 - y) * 2 + core)
    twin = (x, z, y * 2 + 1 - core)

    def z_peer(d):
        return (x, (z + d) % count_ci, cj)

    def remote(src, dst, send, recv, device):
        return pltpu.make_async_remote_copy(
            src_ref=src, dst_ref=dst, send_sem=send, recv_sem=recv,
            device_id=device, device_id_type=MESH,
        )

    def load(c):
        start = c * WIDTH
        if not isinstance(c, int):
            start = pl.multiple_of(start, WIDTH)
        return pltpu.make_async_copy(
            mat_ref.at[:, pl.ds(start, WIDTH)], buf.at[0, c], load_sem.at[c]
        )

    def half(h):
        return pl.ds(h * part_rows, part_rows)

    def y_copy(c, h):
        return remote(
            buf.at[0, c, half(h)], buf.at[1, c, half(h)], y_send.at[c, h], y_recv.at[c, h], y_peer
        )

    def x_copy(c, h):
        return remote(
            buf.at[1 - off, c, half(h)], xb.at[c, half(h)], x_send.at[c, h], x_recv.at[c, h], x_peer
        )

    def a_copy(c):
        return remote(buf.at[off, c], pa.at[c], a_send.at[c], a_recv.at[c], twin)

    def f_copy(c, h):
        return remote(
            xb.at[c, half(h)], px.at[c, half(h)], f_send.at[c, h], f_recv.at[c, h], twin
        )

    q_in = pltpu.make_async_copy(mat_ref.at[:, pl.ds(0, WIDTH)], qa.at[z], q_load)
    q_in.start()
    for c in range(chunks):
        load(c).start()

    barrier = pltpu.get_barrier_semaphore()
    peers = [x_peer, y_peer, twin] + [z_peer(d) for d in range(1, count_ci)]
    for peer in peers:
        pl.semaphore_signal(barrier, inc=1, device_id=peer, device_id_type=MESH)
    pl.semaphore_wait(barrier, len(peers))

    qx_copy = remote(qa.at[z], qx.at[z], qx_sems.at[0], qx_sems.at[1], x_peer)
    sx_copy = remote(sample_ref, sx, sx_sems.at[0], sx_sems.at[1], x_peer)

    def qa_copy(d, slot):
        return remote(qa.at[z], qa.at[slot], qa_send.at[d], qa_recv.at[d], z_peer(d))

    def qz_copy(d, slot):
        return remote(qx.at[z], qx.at[slot], qz_send.at[d], qz_recv.at[d], z_peer(d))

    def send_own(c):
        load(c).wait()
        for h in range(2):
            y_copy(c, h).start()

        @pl.when(off == 1)
        def _():
            for h in range(2):
                x_copy(c, h).start()

    q_in.wait()
    qx_copy.start()
    for c in range(AHEAD):
        send_own(c)
    sx_copy.start()
    for d in range(1, count_ci):
        qa_copy(d, z).start()
    def relay(c, h):
        y_copy(c, h).wait_recv()

        @pl.when(off == 0)
        def _():
            x_copy(c, h).start()

        if h == 1:
            a_copy(c).start()

            @pl.when(c + AHEAD < chunks)
            def _():
                send_own(c + AHEAD)

    def forward(c, h):
        x_copy(c, h).wait_recv()
        f_copy(c, h).start()

    def compute(k):
        a_copy(k).wait_recv()
        for h in range(2):
            f_copy(k, h).wait_recv()
        own = jnp.concatenate([jnp.transpose(buf[off, k]), jnp.transpose(xb[k])], axis=1)
        other = jnp.concatenate([jnp.transpose(pa[k]), jnp.transpose(px[k])], axis=1)
        both = jnp.concatenate([own, other], axis=0)
        squares = jnp.sum(both * both, axis=1, keepdims=True)
        inverse = 1.0 / jnp.sqrt(squares + EPS)
        high, low = split(both)
        left = jnp.concatenate([high, low, high], axis=1)
        product = jnp.dot(left, qmat[...], preferred_element_type=jnp.float32) * inverse
        for part in range(2):
            home = core if part == 0 else 1 - core
            first = (home * slab + k * WIDTH) * (group // WIDTH)
            for t in range(group // WIDTH):
                out_ref[pl.ds(first + t, WIDTH, stride=group // WIDTH), :] = product[
                    part * WIDTH:(part + 1) * WIDTH, t * WIDTH:(t + 1) * WIDTH
                ]

    def inverses_of_queries():
        for d in range(1, count_ci):
            slot = (z + count_ci - d) % count_ci
            qa_copy(d, slot).wait_recv()
            qz_copy(d, slot).wait_recv()
        sx_copy.wait_recv()
        inverses = []
        for i in range(count_ci):
            first, second = qa[i], qx[i]
            squares = jnp.sum(first * first, axis=0, keepdims=True)
            squares += jnp.sum(second * second, axis=0, keepdims=True)
            inverses.append(1.0 / jnp.sqrt(squares + EPS))
        return inverses

    def prepare(side, pieces, picks, inverses):
        lane = lax.broadcasted_iota(jnp.int32, (rows, WIDTH), 1)
        row = picks[pl.ds(cj, 1), :].astype(jnp.float32)
        mask = jnp.transpose(jnp.broadcast_to(row, (WIDTH, rows)))
        tiles = [jnp.zeros((rows, WIDTH), jnp.float32)] * (group // WIDTH)
        for i in range(count_ci):
            value = pieces[i] * inverses[i] * KEEP * mask
            first = i * query_slab
            if first % WIDTH:
                value = pltpu.roll(value, first % WIDTH, 1)
            for t in range(first // WIDTH, (first + query_slab - 1) // WIDTH + 1):
                low_lane, high_lane = first - t * WIDTH, first + query_slab - t * WIDTH
                tiles[t] = jnp.where((lane >= low_lane) & (lane < high_lane), value, tiles[t])
        for t, tile in enumerate(tiles):
            high, low = split(tile)
            where = slice(t * WIDTH, (t + 1) * WIDTH)
            for third, piece in enumerate((high, high, low)):
                base = third * 2 * rows + side * rows
                qmat[base:base + rows, where] = piece

    def both_halves(step, c):
        step(c, 0)
        step(c, 1)

    relay(0, 0)
    qx_copy.wait_recv()
    for d in range(1, count_ci):
        qz_copy(d, z).start()
    relay(0, 1)

    lag = chunks * 3 // 8

    @pl.loop(1, lag)
    def _(c):
        both_halves(relay, c)
        both_halves(forward, c - 1)

    relay(lag, 0)
    inverses = inverses_of_queries()
    relay(lag, 1)
    both_halves(forward, lag - 1)
    prepare(0, qa, sample_ref, inverses)
    relay(lag + 1, 0)
    prepare(1, qx, sx, inverses)
    relay(lag + 1, 1)
    both_halves(forward, lag)

    @pl.loop(lag + 2, 2 * lag + 2)
    def _(c):
        k = 2 * (c - lag - 2)
        relay(c, 0)
        compute(k)
        relay(c, 1)
        both_halves(forward, c - 1)
        compute(k + 1)

    @pl.loop(2 * lag + 2, chunks)
    def _(c):
        both_halves(relay, c)
        both_halves(forward, c - 1)
        compute(c - 2)

    forward(chunks - 1, 0)
    compute(chunks - 2)
    forward(chunks - 1, 1)
    compute(chunks - 1)

    @pl.loop(0, chunks)
    def _(c):
        a_copy(c).wait_send()
        for h in range(2):
            y_copy(c, h).wait_send()
            x_copy(c, h).wait_send()
            f_copy(c, h).wait_send()

    qx_copy.wait_send()
    sx_copy.wait_send()
    for d in range(1, count_ci):
        qa_copy(d, z).wait_send()
        qz_copy(d, z).wait_send()


def fused(matrix, sample):
    count_ci, count_cj = lax.axis_size("ci"), lax.axis_size("cj")
    rows, slab = matrix.shape
    query_slab = QUERY // (count_ci * count_cj)
    group = query_slab * count_ci
    chunks = slab // WIDTH
    dma = pltpu.SemaphoreType.DMA
    blocks = pltpu.VMEM((chunks, rows, WIDTH), jnp.float32)
    pieces = pltpu.VMEM((count_ci, rows, WIDTH), jnp.float32)
    result = pl.pallas_call(
        functools.partial(kernel, count_ci, chunks, query_slab),
        out_shape=pltpu.VMEM((2 * slab * group // WIDTH, WIDTH), jnp.float32),
        in_specs=[
            pl.BlockSpec(memory_space=pltpu.HBM),
            pl.BlockSpec(memory_space=pltpu.VMEM),
        ],
        out_specs=pl.BlockSpec(memory_space=pltpu.VMEM),
        scratch_shapes=[
            pltpu.VMEM((2, chunks, rows, WIDTH), jnp.float32),
            blocks, blocks, blocks, pieces, pieces,
            pltpu.VMEM(sample.shape[1:], sample.dtype),
            pltpu.VMEM((6 * rows, group), jnp.bfloat16),
        ] + [dma((chunks,))] + [dma((chunks, 2))] * 4 + [dma((chunks,))] * 2
        + [dma((chunks, 2))] * 2 + [dma, dma((2,)), dma((2,))] + [dma((count_ci,))] * 4,
        compiler_params=pltpu.CompilerParams(
            collective_id=0, has_side_effects=True, vmem_limit_bytes=56_000_000
        ),
    )(matrix, sample[0])
    return result.reshape(1, 2 * slab, 1, group)


def solution(mesh):
    in_specs = (P("rows", ("ci", "cj")), P("ci", None, "rows"))
    out_specs = P("ci", "rows", "cj", None)
    body = fused if mesh.shape["rows"] == 2 and mesh.shape["cj"] == 4 else shards
    return jax.shard_map(body, mesh=mesh, in_specs=in_specs, out_specs=out_specs, check_vma=False)
```

```python
import functools

import jax
import jax.numpy as jnp
from jax import lax
from jax.experimental import pallas as pl
from jax.experimental.pallas import tpu as pltpu
from jax.sharding import PartitionSpec as P

QUERY = 1536


EPS = 1e-06
KEEP = 2.0

WIDTH = 128
AHEAD = 2
MESH = pl.DeviceIdType.MESH


def shards(matrix, sample):
    local_squares = jnp.sum(matrix * matrix, axis=0)
    total_squares = lax.psum(local_squares, "rows")
    inverse = 1.0 / jnp.sqrt(total_squares + EPS)
    unit = matrix * inverse[None, :]
    count_ci = lax.axis_size("ci")
    count_cj = lax.axis_size("cj")
    count_rows = lax.axis_size("rows")
    row_count = matrix.shape[0]
    query_slab = QUERY // (count_ci * count_cj)
    queries = unit[:, :query_slab] * KEEP
    swapped = lax.all_to_all(unit, "cj", split_axis=0, concat_axis=1, tiled=True)
    ranged = lax.all_to_all(swapped, "rows", split_axis=1, concat_axis=0, tiled=True)
    columns = lax.all_gather(ranged, "cj", axis=0, tiled=True)
    picks = lax.dynamic_index_in_dim(sample[0], lax.axis_index("cj"), 0, keepdims=False).astype(
        jnp.float32
    )
    part_group = lax.all_gather(queries, "ci", axis=1, tiled=True) * picks[:, None]
    masked = lax.all_gather(part_group, "rows", axis=0, tiled=True)
    group_width = masked.shape[1]
    reordered = masked.reshape(count_rows, count_cj, row_count // count_cj, group_width)
    reordered = jnp.transpose(reordered, (1, 0, 2, 3)).reshape(count_rows * row_count, group_width)
    result = jnp.dot(
        jnp.transpose(columns),
        reordered,
        precision=lax.Precision.HIGHEST,
        preferred_element_type=jnp.float32,
    )
    return result[None, :, None, :]


def split(value):
    high = value.astype(jnp.bfloat16)
    low = (value - high.astype(jnp.float32)).astype(jnp.bfloat16)
    return high, low


def kernel(
    count_ci, chunks, query_slab,
    mat_ref, sample_ref, out_ref,
    buf, xb, pa, px, qa, qx, sx, qmat,
    load_sem, y_send, y_recv, x_send, x_recv, a_send, a_recv, f_send, f_recv,
    q_load, qx_sems, sx_sems, qa_send, qa_recv, qz_send, qz_recv,
):
    x, z, cj = lax.axis_index("rows"), lax.axis_index("ci"), lax.axis_index("cj")
    y, core = cj // 2, cj % 2
    off = (x + y) % 2
    rows = mat_ref.shape[0]
    slab = chunks * WIDTH
    group = query_slab * count_ci
    part_rows = rows // 2
    x_peer = (1 - x, z, cj)
    y_peer = (x, z, (1 - y) * 2 + core)
    twin = (x, z, y * 2 + 1 - core)

    def z_peer(d):
        return (x, (z + d) % count_ci, cj)

    def remote(src, dst, send, recv, device):
        return pltpu.make_async_remote_copy(
            src_ref=src, dst_ref=dst, send_sem=send, recv_sem=recv,
            device_id=device, device_id_type=MESH,
        )

    def load(c):
        start = c * WIDTH
        if not isinstance(c, int):
            start = pl.multiple_of(start, WIDTH)
        return pltpu.make_async_copy(
            mat_ref.at[:, pl.ds(start, WIDTH)], buf.at[0, c], load_sem.at[c]
        )

    def half(h):
        return pl.ds(h * part_rows, part_rows)

    def y_copy(c, h):
        return remote(
            buf.at[0, c, half(h)], buf.at[1, c, half(h)], y_send.at[c, h], y_recv.at[c, h], y_peer
        )

    def x_copy(c, h):
        return remote(
            buf.at[1 - off, c, half(h)], xb.at[c, half(h)], x_send.at[c, h], x_recv.at[c, h], x_peer
        )

    def a_copy(c):
        return remote(buf.at[off, c], pa.at[c], a_send.at[c], a_recv.at[c], twin)

    def f_copy(c, h):
        return remote(
            xb.at[c, half(h)], px.at[c, half(h)], f_send.at[c, h], f_recv.at[c, h], twin
        )

    q_in = pltpu.make_async_copy(mat_ref.at[:, pl.ds(0, WIDTH)], qa.at[z], q_load)
    q_in.start()
    for c in range(chunks):
        load(c).start()

    barrier = pltpu.get_barrier_semaphore()
    peers = [x_peer, y_peer, twin] + [z_peer(d) for d in range(1, count_ci)]
    for peer in peers:
        pl.semaphore_signal(barrier, inc=1, device_id=peer, device_id_type=MESH)
    pl.semaphore_wait(barrier, len(peers))

    qx_copy = remote(qa.at[z], qx.at[z], qx_sems.at[0], qx_sems.at[1], x_peer)
    sx_copy = remote(sample_ref, sx, sx_sems.at[0], sx_sems.at[1], x_peer)

    def qa_copy(d, slot):
        return remote(qa.at[z], qa.at[slot], qa_send.at[d], qa_recv.at[d], z_peer(d))

    def qz_copy(d, slot):
        return remote(qx.at[z], qx.at[slot], qz_send.at[d], qz_recv.at[d], z_peer(d))

    def send_own(c):
        load(c).wait()
        for h in range(2):
            y_copy(c, h).start()

        @pl.when(off == 1)
        def _():
            for h in range(2):
                x_copy(c, h).start()

    q_in.wait()
    qx_copy.start()
    for c in range(AHEAD):
        send_own(c)
    sx_copy.start()
    for d in range(1, count_ci):
        qa_copy(d, z).start()
    def relay(c, h):
        y_copy(c, h).wait_recv()

        @pl.when(off == 0)
        def _():
            x_copy(c, h).start()

        if h == 1:
            a_copy(c).start()

            @pl.when(c + AHEAD < chunks)
            def _():
                send_own(c + AHEAD)

    def forward(c, h):
        x_copy(c, h).wait_recv()
        f_copy(c, h).start()

    def compute(k):
        a_copy(k).wait_recv()
        for h in range(2):
            f_copy(k, h).wait_recv()
        own = jnp.concatenate([jnp.transpose(buf[off, k]), jnp.transpose(xb[k])], axis=1)
        other = jnp.concatenate([jnp.transpose(pa[k]), jnp.transpose(px[k])], axis=1)
        both = jnp.concatenate([own, other], axis=0)
        squares = jnp.sum(both * both, axis=1, keepdims=True)
        inverse = 1.0 / jnp.sqrt(squares + EPS)
        high, low = split(both)
        left = jnp.concatenate([high, low, high], axis=1)
        product = jnp.dot(left, qmat[...], preferred_element_type=jnp.float32) * inverse
        for part in range(2):
            home = core if part == 0 else 1 - core
            first = (home * slab + k * WIDTH) * (group // WIDTH)
            for t in range(group // WIDTH):
                out_ref[pl.ds(first + t, WIDTH, stride=group // WIDTH), :] = product[
                    part * WIDTH:(part + 1) * WIDTH, t * WIDTH:(t + 1) * WIDTH
                ]

    def inverses_of_queries():
        for d in range(1, count_ci):
            slot = (z + count_ci - d) % count_ci
            qa_copy(d, slot).wait_recv()
            qz_copy(d, slot).wait_recv()
        sx_copy.wait_recv()
        inverses = []
        for i in range(count_ci):
            first, second = qa[i], qx[i]
            squares = jnp.sum(first * first, axis=0, keepdims=True)
            squares += jnp.sum(second * second, axis=0, keepdims=True)
            inverses.append(1.0 / jnp.sqrt(squares + EPS))
        return inverses

    def prepare(side, pieces, picks, inverses):
        lane = lax.broadcasted_iota(jnp.int32, (rows, WIDTH), 1)
        row = picks[pl.ds(cj, 1), :].astype(jnp.float32)
        mask = jnp.transpose(jnp.broadcast_to(row, (WIDTH, rows)))
        tiles = [jnp.zeros((rows, WIDTH), jnp.float32)] * (group // WIDTH)
        for i in range(count_ci):
            value = pieces[i] * inverses[i] * KEEP * mask
            first = i * query_slab
            if first % WIDTH:
                value = pltpu.roll(value, first % WIDTH, 1)
            for t in range(first // WIDTH, (first + query_slab - 1) // WIDTH + 1):
                low_lane, high_lane = first - t * WIDTH, first + query_slab - t * WIDTH
                tiles[t] = jnp.where((lane >= low_lane) & (lane < high_lane), value, tiles[t])
        for t, tile in enumerate(tiles):
            high, low = split(tile)
            where = slice(t * WIDTH, (t + 1) * WIDTH)
            for third, piece in enumerate((high, high, low)):
                base = third * 2 * rows + side * rows
                qmat[base:base + rows, where] = piece

    def both_halves(step, c):
        step(c, 0)
        step(c, 1)

    relay(0, 0)
    qx_copy.wait_recv()
    for d in range(1, count_ci):
        qz_copy(d, z).start()
    relay(0, 1)

    lag = chunks * 3 // 8

    @pl.loop(1, lag)
    def _(c):
        both_halves(relay, c)
        both_halves(forward, c - 1)

    relay(lag, 0)
    inverses = inverses_of_queries()
    relay(lag, 1)
    both_halves(forward, lag - 1)
    prepare(0, qa, sample_ref, inverses)
    relay(lag + 1, 0)
    prepare(1, qx, sx, inverses)
    relay(lag + 1, 1)
    both_halves(forward, lag)

    @pl.loop(lag + 2, 2 * lag + 2)
    def _(c):
        k = 2 * (c - lag - 2)
        relay(c, 0)
        compute(k)
        relay(c, 1)
        both_halves(forward, c - 1)
        compute(k + 1)

    @pl.loop(2 * lag + 2, chunks)
    def _(c):
        both_halves(relay, c)
        both_halves(forward, c - 1)
        compute(c - 2)

    forward(chunks - 1, 0)
    compute(chunks - 2)
    forward(chunks - 1, 1)
    compute(chunks - 1)

    @pl.loop(0, chunks)
    def _(c):
        a_copy(c).wait_send()
        for h in range(2):
            y_copy(c, h).wait_send()
            x_copy(c, h).wait_send()
            f_copy(c, h).wait_send()

    qx_copy.wait_send()
    sx_copy.wait_send()
    for d in range(1, count_ci):
        qa_copy(d, z).wait_send()
        qz_copy(d, z).wait_send()


def fused(matrix, sample):
    count_ci, count_cj = lax.axis_size("ci"), lax.axis_size("cj")
    rows, slab = matrix.shape
    query_slab = QUERY // (count_ci * count_cj)
    group = query_slab * count_ci
    chunks = slab // WIDTH
    dma = pltpu.SemaphoreType.DMA
    blocks = pltpu.VMEM((chunks, rows, WIDTH), jnp.float32)
    pieces = pltpu.VMEM((count_ci, rows, WIDTH), jnp.float32)
    result = pl.pallas_call(
        functools.partial(kernel, count_ci, chunks, query_slab),
        out_shape=pltpu.VMEM((2 * slab * group // WIDTH, WIDTH), jnp.float32),
        in_specs=[
            pl.BlockSpec(memory_space=pltpu.HBM),
            pl.BlockSpec(memory_space=pltpu.VMEM),
        ],
        out_specs=pl.BlockSpec(memory_space=pltpu.VMEM),
        scratch_shapes=[
            pltpu.VMEM((2, chunks, rows, WIDTH), jnp.float32),
            blocks, blocks, blocks, pieces, pieces,
            pltpu.VMEM(sample.shape[1:], sample.dtype),
            pltpu.VMEM((6 * rows, group), jnp.bfloat16),
        ] + [dma((chunks,))] + [dma((chunks, 2))] * 4 + [dma((chunks,))] * 2
        + [dma((chunks, 2))] * 2 + [dma, dma((2,)), dma((2,))] + [dma((count_ci,))] * 4,
        compiler_params=pltpu.CompilerParams(
            collective_id=0, has_side_effects=True, vmem_limit_bytes=56_000_000
        ),
    )(matrix, sample[0])
    return result.reshape(1, 2 * slab, 1, group)


def solution(mesh):
    in_specs = (P("rows", ("ci", "cj")), P("ci", None, "rows"))
    out_specs = P("ci", "rows", "cj", None)
    body = fused if mesh.shape["rows"] == 2 and mesh.shape["cj"] == 4 else shards
    return jax.shard_map(body, mesh=mesh, in_specs=in_specs, out_specs=out_specs, check_vma=False)
```
